32 devices in a mesh: section: 8 (over z, core), tm: 4 (over y, x).
Axes of the slice: x: 2, y: 2, z: 4, core: 2. Of those that a mesh axis runs over, the one named last changes fastest.
Arguments:
- frames: bfloat16 [4, 256, 1024], P(None, 'tm'), may hold values from -6 to 6, as said below
- lengths: int32 [4], replicated, may hold values from 64 to 256
- ffn_gain: float32 [8, 1024], P('section'), may hold values from 0.1 to 1.9
- ffn_up: bfloat16 [8, 1024, 2048], P('section'), may hold values from -0.1875 to 0.1875
- ffn_down: bfloat16 [8, 2048, 1024], P('section'), may hold values from -0.125 to 0.125
- attn_gain: float32 [8, 1024], P('section'), may hold values from 0.1 to 1.9
- query_weight: bfloat16 [8, 1024, 1024], P('section'), may hold values from -8 to 8
- key_weight: bfloat16 [8, 1024, 1024], P('section'), may hold values from -0.1875 to 0.1875
- value_weight: bfloat16 [8, 1024, 1024], P('section'), may hold values from -0.1875 to 0.1875
- out_weight: bfloat16 [8, 1024, 1024], P('section'), may hold values from -0.1875 to 0.1875
- conv_gain: float32 [8, 1024], P('section'), may hold values from 0.1 to 1.9
- expand_weight: bfloat16 [8, 1024, 2048], P('section'), may hold values from -0.1875 to 0.1875
- depth_weight: float32 [8, 31, 1024], P('section'), may hold values from -1 to 1
- depth_gain: float32 [8, 1024], P('section'), may hold values from 0.1 to 1.9
- norm_shift: float32 [8, 1024], P('section'), may hold values from -0.5 to 0.5
- shrink_weight: bfloat16 [8, 1024, 1024], P('section'), may hold values from -0.1875 to 0.1875
- final_gain: float32 [8, 1024], P('section'), may hold values from 0.1 to 1.9
Outputs:
- hidden_states: bfloat16 [8, 4, 256, 1024], P('section', None, 'tm')
The draws below stay inside these ranges and needn't reach their ends.
Inputs may be any that keep to these rules, and one draw needn't show every extreme that they name: `frames`: input features of order one.
All inputs are finite; a program needn't handle non-finite values.
Results may differ from the reference program's by a relative error of at most 0.02.
Values may be sent and summed in bfloat16 or wider, within the bound.
No kernel may reach another device: no remote copies, remote signals or barrier semaphores. Data moves between devices by JAX's collectives and lax.ppermute only.
A program may use at most 128 MiB of HBM per device.

```python
import jax
import jax.numpy as jnp
from jax import lax

D = 1024
HEADS = 16
HEAD = 64
KERNEL = 31
FF = 2048
MICRO = 4
SECTIONS = 8
LEN = 256


def shared_projection(key):
    base = jax.random.normal(jax.random.fold_in(key, 101), (SECTIONS, D, D), jnp.float32) * D ** (-0.5)
    own = jax.random.normal(jax.random.fold_in(key, 102), (SECTIONS, D, D), jnp.float32) * D ** (-0.5)
    base = jnp.clip(base, -6.0 / 32.0, 6.0 / 32.0)
    own = jnp.clip(own, -6.0 / 32.0, 6.0 / 32.0)
    return (base, own)


def draw_key_weight(key, part):
    base, own = shared_projection(key)
    return base.astype(jnp.bfloat16)


def draw_query_weight(key, part):
    base, own = shared_projection(key)
    grades = jax.random.randint(jax.random.fold_in(key, 104), (SECTIONS, HEADS), 0, 4)
    drawn = jnp.where(grades > 0, 0.25 * jnp.exp2(grades.astype(jnp.float32)), 0.0)
    drawn = jnp.repeat(drawn, HEAD, axis=1)[:, None, :]
    result = base * drawn + own
    return jnp.clip(result, -8.0, 8.0).astype(jnp.bfloat16)


def draw_frames(key, part):
    values = jax.random.normal(jax.random.fold_in(key, 201), (MICRO, LEN, D), jnp.float32)
    return jnp.clip(values, -6.0, 6.0).astype(jnp.bfloat16)


def touch_ends(values, stream_key, low, high):
    shape = values.shape
    index_at = [jax.random.randint(jax.random.fold_in(stream_key, axis), (), 0, shape[axis]) for axis in range(len(shape))]
    values = values.at[tuple(index_at)].set(low)
    longest = shape.index(max(shape))
    index_at[longest] = (index_at[longest] + 1) % shape[longest]
    return values.at[tuple(index_at)].set(high)


def steps_of(own_key, extent, split, least, high):
    def one(axis_at, shards_of):
        draws = jax.random.uniform(jax.random.fold_in(jax.random.fold_in(own_key, 6), axis_at), (shards_of,), jnp.float32, least / len(split), high / len(split))
        return jnp.repeat(jnp.exp(draws), extent[axis_at] // shards_of).reshape((-1,) + (1,) * (len(extent) - axis_at - 1))

    factor_of = one(*split[0])
    for cut in split[1:]:
        factor_of = factor_of * one(*cut)
    return factor_of


def normal_values(stream_key, extent, deviation, limit, split=(), kind=jnp.bfloat16):
    values = deviation * jax.random.normal(stream_key, extent, jnp.float32)
    if split:
        values = values * steps_of(stream_key, extent, split, -0.22, 0.18)
    return jnp.clip(values, -limit, limit).astype(kind)


def setup_inputs(seed: int = 0) -> dict:
    seeds = jax.random.split(jax.random.key(seed), 18)
    frames = draw_frames(jax.random.fold_in(seeds[17], 71), 0)
    lengths = touch_ends(jax.random.randint(seeds[1], (MICRO,), LEN // 4, LEN + 1), jax.random.fold_in(seeds[1], 1), LEN // 4, LEN).astype(jnp.int32)
    ffn_gain = jnp.clip(1.0 + 0.18 * jax.random.normal(seeds[2], (SECTIONS, D), jnp.float32), 0.1, 1.9)
    ffn_up = normal_values(seeds[3], (SECTIONS, D, FF), D ** -0.5, 0.1875, ((0, 8),))
    ffn_down = normal_values(seeds[4], (SECTIONS, FF, D), FF ** -0.5, 0.125, ((0, 8),))
    attn_gain = jnp.clip(1.0 + 0.18 * jax.random.normal(seeds[5], (SECTIONS, D), jnp.float32), 0.1, 1.9)
    query_weight = draw_query_weight(jax.random.fold_in(seeds[17], 71), 0)
    key_weight = draw_key_weight(jax.random.fold_in(seeds[17], 71), 0)
    value_weight = normal_values(seeds[8], (SECTIONS, D, D), D ** -0.5, 0.1875, ((0, 8),))
    out_weight = normal_values(seeds[9], (SECTIONS, D, D), D ** -0.5, 0.1875, ((0, 8),))
    conv_gain = jnp.clip(1.0 + 0.18 * jax.random.normal(seeds[10], (SECTIONS, D), jnp.float32), 0.1, 1.9)
    expand_weight = normal_values(seeds[11], (SECTIONS, D, 2 * D), D ** -0.5, 0.1875, ((0, 8),))
    depth_weight = normal_values(seeds[12], (SECTIONS, KERNEL, D), KERNEL ** -0.5, 1.0, ((0, 8),), jnp.float32)
    depth_gain = jnp.clip(1.0 + 0.18 * jax.random.normal(seeds[13], (SECTIONS, D), jnp.float32), 0.1, 1.9)
    norm_shift = jnp.clip(jax.random.uniform(seeds[14], (SECTIONS, D), jnp.float32, -0.5, 0.5) * steps_of(seeds[14], (SECTIONS, D), ((0, 8),), -0.4, 0.0), -0.5, 0.5)
    shrink_weight = normal_values(seeds[15], (SECTIONS, D, D), D ** -0.5, 0.1875, ((0, 8),))
    final_gain = jnp.clip(1.0 + 0.18 * jax.random.normal(seeds[16], (SECTIONS, D), jnp.float32), 0.1, 1.9)
    return {"frames": frames, "lengths": lengths, "ffn_gain": ffn_gain, "ffn_up": ffn_up, "ffn_down": ffn_down, "attn_gain": attn_gain, "query_weight": query_weight, "key_weight": key_weight, "value_weight": value_weight, "out_weight": out_weight, "conv_gain": conv_gain, "expand_weight": expand_weight, "depth_weight": depth_weight, "depth_gain": depth_gain, "norm_shift": norm_shift, "shrink_weight": shrink_weight, "final_gain": final_gain}


EPS = 1e-05

def normalize(value, gain):
    mean = lax.optimization_barrier(jnp.mean(value, axis=-1, keepdims=True))
    centred = value - mean
    spread = lax.optimization_barrier(jnp.mean(centred * centred, axis=-1, keepdims=True))
    return centred * lax.rsqrt(spread + EPS) * gain

def block(inputs, length, weights):
    ffn_gain, ffn_up, ffn_down, attn_gain, query_weight, key_weight, value_weight, out_weight, conv_gain, expand_weight, depth_weight, depth_gain, norm_shift, shrink_weight, final_gain = weights
    positions = jnp.arange(LEN, dtype=jnp.int32)
    keep = positions < length
    ffn_normed = normalize(inputs.astype(jnp.float32), ffn_gain).astype(jnp.bfloat16)
    inner = jax.nn.silu(jnp.dot(ffn_normed, ffn_up, preferred_element_type=jnp.float32)).astype(jnp.bfloat16)
    start = inputs.astype(jnp.float32) + 0.5 * jnp.dot(inner, ffn_down, preferred_element_type=jnp.float32)
    normed = normalize(start, attn_gain).astype(jnp.bfloat16)
    queries = jnp.dot(normed, query_weight, preferred_element_type=jnp.float32).astype(jnp.bfloat16)
    keys = jnp.dot(normed, key_weight, preferred_element_type=jnp.float32).astype(jnp.bfloat16)
    values = jnp.dot(normed, value_weight, preferred_element_type=jnp.float32).astype(jnp.bfloat16)
    scale = 1.0 / HEAD ** 0.5

    def one_head(index):
        begin = (index * HEAD).astype(jnp.int32)
        q_head = lax.dynamic_slice_in_dim(queries, begin, HEAD, 1)
        k_head = lax.dynamic_slice_in_dim(keys, begin, HEAD, 1)
        v_head = lax.dynamic_slice_in_dim(values, begin, HEAD, 1)
        scores = jnp.dot(q_head, k_head.T, preferred_element_type=jnp.float32) * scale
        scores = jnp.where(keep[None, :], scores, -1e+30)
        peak = lax.optimization_barrier(jnp.max(scores, axis=-1, keepdims=True))
        weights_h = jnp.exp(scores - peak)
        total = lax.optimization_barrier(jnp.sum(weights_h, axis=-1, keepdims=True))
        mixed = jnp.dot(weights_h.astype(jnp.bfloat16), v_head, preferred_element_type=jnp.float32)
        return (mixed / total).astype(jnp.bfloat16)
    per_head = lax.map(one_head, jnp.arange(HEADS, dtype=jnp.int32))
    context = jnp.transpose(per_head, (1, 0, 2)).reshape(LEN, D)
    mid = start + jnp.dot(context, out_weight, preferred_element_type=jnp.float32)
    conv_in = normalize(mid, conv_gain).astype(jnp.bfloat16)
    expanded = jnp.dot(conv_in, expand_weight, preferred_element_type=jnp.float32)
    glu = expanded[:, :D] * jax.nn.sigmoid(expanded[:, D:]) * keep[:, None].astype(jnp.float32)
    glu = glu.astype(jnp.bfloat16)
    rim = KERNEL // 2
    padded = jnp.pad(glu, ((rim, rim), (0, 0))).astype(jnp.float32)
    depth = jnp.zeros((LEN, D), jnp.float32)
    for offset in range(KERNEL):
        depth = depth + padded[offset:offset + LEN] * depth_weight[offset]
    shifted = normalize(depth, depth_gain) + norm_shift
    swished = (shifted * jax.nn.sigmoid(shifted)).astype(jnp.bfloat16)
    closing = mid + jnp.dot(swished, shrink_weight, preferred_element_type=jnp.float32)
    return normalize(closing, final_gain).astype(jnp.bfloat16)

def reference(frames, lengths, ffn_gain, ffn_up, ffn_down, attn_gain, query_weight, key_weight, value_weight, out_weight, conv_gain, expand_weight, depth_weight, depth_gain, norm_shift, shrink_weight, final_gain):
    stacked = (ffn_gain, ffn_up, ffn_down, attn_gain, query_weight, key_weight, value_weight, out_weight, conv_gain, expand_weight, depth_weight, depth_gain, norm_shift, shrink_weight, final_gain)

    def section_step(current, weights):
        result = lax.map(lambda pair: block(pair[0], pair[1], weights), (current, lengths))
        return (result, result)
    finished, hidden_states = lax.scan(section_step, frames, stacked)
    return hidden_states
```

```python
import math

import jax
import jax.numpy as jnp
from jax import lax
from jax.experimental import pallas as pl
from jax.experimental.pallas import tpu as pltpu
from jax.sharding import PartitionSpec as P

HEADS = 16
EPS = 1e-05
LANES = 128
F32 = jnp.float32
BF16 = jnp.bfloat16


def sigmoid(value):
    return 0.5 * jnp.tanh(0.5 * value) + 0.5


def normalize(value, gain):
    mean = jnp.mean(value, axis=-1, keepdims=True)
    centred = value - mean
    spread = jnp.mean(centred * centred, axis=-1, keepdims=True)
    return centred * lax.rsqrt(spread + EPS) * gain


def dot(left, right):
    return jnp.dot(left, right, preferred_element_type=F32)


def block_kernel(heads, kernel, cols):
    def run(
        info,
        inputs,
        small,
        up,
        down,
        query,
        key,
        value,
        out,
        expand,
        shrink,
        kept,
        result,
        x_s,
        small_s,
        up_s,
        down_s,
        query_s,
        key_s,
        value_s,
        out_s,
        expand_s,
        shrink_s,
        norm_s,
        inner_s,
        start_s,
        q_s,
        k_s,
        v_s,
        glu_s,
        depth_s,
        sems,
    ):
        length, width = x_s.shape
        hidden = inner_s.shape[1]
        head = width // heads
        rim = kernel // 2
        pad = (glu_s.shape[0] - length) // 2

        @pl.when(info[0] == 1)
        def active():
            copies = []

            def fetch(source, target):
                copy = pltpu.make_async_copy(source, target, sems.at[len(copies)])
                copy.start()
                copies.append(copy)
                return copy

            get_x = fetch(inputs, x_s)
            get_small = fetch(small, small_s)
            get_up = [
                fetch(up.at[0, :, pl.ds(j, cols)], up_s.at[:, pl.ds(j, cols)])
                for j in range(0, hidden, cols)
            ]
            get_down = fetch(down.at[0], down_s)
            get_query = fetch(query.at[0], query_s)
            get_key = fetch(key.at[0], key_s)
            get_value = fetch(value.at[0], value_s)
            get_out = fetch(out.at[0], out_s)
            get_expand = fetch(expand.at[0], expand_s)
            get_shrink = fetch(shrink.at[0], shrink_s)

            step = 32

            def rows_loop(fn):
                def one(i, carry):
                    fn(pl.ds(pl.multiple_of(i * step, step), step))
                    return carry

                lax.fori_loop(0, length // step, one, 0, unroll=2)

            zero = jnp.zeros((pad, width), F32)
            glu_s[0:pad, :] = zero
            glu_s[pad + length : pad + length + pad, :] = zero

            get_x.wait()
            get_small.wait()

            def ffn_norm(at):
                norm_s[at, :] = normalize(x_s[at, :].astype(F32), small_s[0:1, :]).astype(BF16)

            rows_loop(ffn_norm)
            for index, j in enumerate(range(0, hidden, cols)):
                get_up[index].wait()
                part = dot(norm_s[...], up_s[:, j : j + cols])
                inner_s[:, j : j + cols] = (part * sigmoid(part)).astype(BF16)
            get_down.wait()
            for j in range(0, width, cols):
                part = dot(inner_s[...], down_s[:, j : j + cols])
                start_s[:, j : j + cols] = x_s[:, j : j + cols].astype(F32) + 0.5 * part

            def attn_norm(at):
                norm_s[at, :] = normalize(start_s[at, :], small_s[1:2, :]).astype(BF16)

            rows_loop(attn_norm)
            for get, weight, target in (
                (get_query, query_s, q_s),
                (get_key, key_s, k_s),
                (get_value, value_s, v_s),
            ):
                get.wait()
                for j in range(0, width, cols):
                    target[:, j : j + cols] = dot(norm_s[...], weight[:, j : j + cols]).astype(BF16)

            frames = info[1]
            seen = lax.broadcasted_iota(jnp.int32, (1, length), 1) < frames
            lane = lax.broadcasted_iota(jnp.int32, (1, LANES), 1)
            group = LANES // head
            scale = 1.0 / math.sqrt(head)

            def one_group(g, carry):
                at = pl.ds(pl.multiple_of(g * LANES, LANES), LANES)
                queries, keys, values = q_s[:, at], k_s[:, at], v_s[:, at]
                mixed = jnp.zeros((length, 2 * LANES), F32)
                for h in range(group):
                    mine = (lane >= h * head) & (lane < (h + 1) * head)
                    k_head = jnp.where(mine, keys, jnp.zeros_like(keys))
                    scores = lax.dot_general(
                        queries, k_head, (((1,), (1,)), ((), ())), preferred_element_type=F32
                    )
                    scores = jnp.where(seen, scores * scale, -1e30)
                    peak = jnp.max(scores, axis=-1, keepdims=True)
                    weights = jnp.exp(scores - peak).astype(BF16)
                    v_head = jnp.where(mine, values, jnp.zeros_like(values))
                    ones = jnp.broadcast_to(jnp.where(mine, 1.0, 0.0).astype(BF16), (length, LANES))
                    mixed = mixed + dot(weights, jnp.concatenate([v_head, ones], axis=1))
                norm_s[:, at] = (
                    mixed[:, :LANES] * pl.reciprocal(mixed[:, LANES:], approx=False)
                ).astype(BF16)
                return carry

            lax.fori_loop(0, width // LANES, one_group, 0)

            get_out.wait()
            for j in range(0, width, cols):
                part = dot(norm_s[...], out_s[:, j : j + cols])
                start_s[:, j : j + cols] = start_s[:, j : j + cols] + part

            def conv_norm(at):
                norm_s[at, :] = normalize(start_s[at, :], small_s[2:3, :]).astype(BF16)

            rows_loop(conv_norm)
            get_expand.wait()
            keep = lax.broadcasted_iota(jnp.int32, (length, 1), 0) < frames
            for j in range(0, width, cols // 2):
                part = dot(norm_s[...], expand_s[:, j : j + cols // 2])
                gate = dot(norm_s[...], expand_s[:, width + j : width + j + cols // 2])
                glu = jnp.where(keep, part * sigmoid(gate), 0.0)
                glu_s[pad : pad + length, j : j + cols // 2] = glu.astype(BF16).astype(F32)

            rows = 64
            shift = pad - rim

            def conv(i, carry):
                at = pl.ds(pl.multiple_of((i % (width // LANES)) * LANES, LANES), LANES)
                begin = pl.multiple_of((i // (width // LANES)) * rows, rows)
                wide = glu_s[pl.ds(begin, rows + 2 * pad), at]
                total = jnp.zeros((rows, LANES), F32)
                for r in range(8):
                    taps = [o for o in range(shift, shift + kernel) if o % 8 == r]
                    extent = rows + 8 if r else rows
                    partial = None
                    for o in taps:
                        tap = small_s[pl.ds(6 + o - shift, 1), at]
                        term = wide[o - r : o - r + extent] * tap
                        partial = term if partial is None else partial + term
                    if r:
                        partial = pltpu.roll(partial, extent - r, 0)[:rows]
                    total = total + partial
                depth_s[pl.ds(begin, rows), at] = total
                return carry

            lax.fori_loop(0, (width // LANES) * (length // rows), conv, 0)

            def swish(at):
                shifted = normalize(depth_s[at, :], small_s[3:4, :]) + small_s[4:5, :]
                norm_s[at, :] = (shifted * sigmoid(shifted)).astype(BF16)

            rows_loop(swish)
            get_shrink.wait()
            for j in range(0, width, cols):
                part = dot(norm_s[...], shrink_s[:, j : j + cols])
                start_s[:, j : j + cols] = start_s[:, j : j + cols] + part

            def closing(at):
                x_s[at, :] = normalize(start_s[at, :], small_s[5:6, :]).astype(BF16)

            rows_loop(closing)
            put = pltpu.make_async_copy(x_s, result, sems.at[len(copies)])
            put.start()
            put.wait()

    return run


def block(info, inputs, small, weights, kept, heads, kernel):
    length, width = inputs.shape
    hidden = weights[0].shape[2]
    cols = 512
    pad = 8 * ((kernel // 2 + 8) // 8)
    vmem = [
        ((length, width), BF16),
        (small.shape, F32),
        *((w.shape[1:], BF16) for w in weights),
        ((length, width), BF16),
        ((length, hidden), BF16),
        ((length, width), F32),
        ((length, width), BF16),
        ((length, width), BF16),
        ((length, width), BF16),
        ((length + 2 * pad, width), F32),
        ((length, width), F32),
    ]
    anywhere = pl.BlockSpec(memory_space=pl.ANY)
    return pl.pallas_call(
        block_kernel(heads, kernel, cols),
        out_shape=jax.ShapeDtypeStruct((length, width), BF16),
        in_specs=[pl.BlockSpec(memory_space=pltpu.SMEM)] + [anywhere] * (3 + len(weights)),
        out_specs=anywhere,
        scratch_shapes=[pltpu.VMEM(shape, kind) for shape, kind in vmem]
        + [pltpu.SemaphoreType.DMA((len(weights) + 2 + hidden // cols,))],
        input_output_aliases={3 + len(weights): 0},
        compiler_params=pltpu.CompilerParams(vmem_limit_bytes=60 * 1024 * 1024),
        name="block",
    )(info, inputs, small, *weights, kept)


def body(
    frames,
    lengths,
    ffn_gain,
    ffn_up,
    ffn_down,
    attn_gain,
    query_weight,
    key_weight,
    value_weight,
    out_weight,
    conv_gain,
    expand_weight,
    depth_weight,
    depth_gain,
    norm_shift,
    shrink_weight,
    final_gain,
):
    sections = lax.axis_size("section")
    section_index = lax.axis_index("section")
    group_index = lax.axis_index("tm")
    micro, rows, width = frames.shape
    peers = lax.axis_size("tm")
    share = peers // micro
    assert share * micro == peers
    utterance = group_index // share
    kernel = depth_weight.shape[1]
    weights = (
        ffn_up,
        ffn_down,
        query_weight,
        key_weight,
        value_weight,
        out_weight,
        expand_weight,
        shrink_weight,
    )
    small = jnp.concatenate(
        [ffn_gain, attn_gain, conv_gain, depth_gain, norm_shift, final_gain, depth_weight[0]]
    )
    small = jnp.pad(small, ((0, -small.shape[0] % 8), (0, 0)))
    length = jnp.sum(jnp.where(jnp.arange(micro, dtype=jnp.int32) == utterance, lengths, 0))
    pairs = [(i, i + 1) for i in range(sections - 1)]

    def apply(step, inputs, kept):
        info = jnp.stack([(step == section_index).astype(jnp.int32), length])
        return block(info, inputs, small, weights, kept, HEADS, kernel)

    across = [[u * share + r for u in range(micro)] for r in range(share)] if share > 1 else None
    within = [[u * share + r for r in range(share)] for u in range(micro)]

    def exchange(parts):
        return lax.all_to_all(parts, "tm", 0, 0, axis_index_groups=across, tiled=True)

    own = exchange(frames)
    if share > 1:
        own = lax.all_gather(own, "tm", axis=1, axis_index_groups=within)
    own = own.reshape(micro * share * rows, width)
    kept = apply(0, own, jnp.zeros_like(own))

    def tick(step, kept):
        return apply(step, lax.ppermute(kept, "section", pairs), kept)

    kept = lax.fori_loop(1, sections, tick, kept)
    parts = kept.reshape(micro, share, rows, width)
    if share > 1:
        parts = lax.dynamic_slice_in_dim(parts, group_index % share, 1, 1)
    return exchange(parts[:, 0])[None]


def solution(mesh):
    return jax.shard_map(
        body,
        mesh=mesh,
        in_specs=(
            P(None, "tm", None),
            P(),
            P("section", None),
            P("section", None, None),
            P("section", None, None),
            P("section", None),
            P("section", None, None),
            P("section", None, None),
            P("section", None, None),
            P("section", None, None),
            P("section", None),
            P("section", None, None),
            P("section", None, None),
            P("section", None),
            P("section", None),
            P("section", None, None),
            P("section", None),
        ),
        out_specs=P("section", None, "tm", None),
        check_vma=False,
    )
```

```python
import math

import jax
import jax.numpy as jnp
from jax import lax
from jax.experimental import pallas as pl
from jax.experimental.pallas import tpu as pltpu
from jax.sharding import PartitionSpec as P

HEADS = 16
EPS = 1e-05
LANES = 128
F32 = jnp.float32
BF16 = jnp.bfloat16


def sigmoid(value):
    return 0.5 * jnp.tanh(0.5 * value) + 0.5


def normalize(value, gain):
    mean = jnp.mean(value, axis=-1, keepdims=True)
    centred = value - mean
    spread = jnp.mean(centred * centred, axis=-1, keepdims=True)
    return centred * lax.rsqrt(spread + EPS) * gain


def dot(left, right):
    return jnp.dot(left, right, preferred_element_type=F32)


def block_kernel(heads, kernel, cols, count):
    def run(info, *refs):
        block_body(info, refs[:count], *refs[count:])

    def block_body(
        info,
        pieces,
        small,
        up,
        down,
        query,
        key,
        value,
        out,
        expand,
        shrink,
        kept,
        result,
        norm_s,
        inner_s,
        start_s,
        q_s,
        k_s,
        v_s,
        glu_s,
        depth_s,
        x_s,
    ):
        length, width = result.shape
        hidden = inner_s.shape[1]
        head = width // heads
        rim = kernel // 2
        pad = (glu_s.shape[0] - length) // 2

        @pl.when(info[0] == 1)
        def active():
            step = 32
            span = min(length, 256)

            def rows_loop(fn):
                def one(i, carry):
                    for j in range(0, span, step):
                        begin = j if span == length else pl.multiple_of(i * span + j, step)
                        fn(pl.ds(begin, step))
                    return carry

                if span == length:
                    one(0, 0)
                else:
                    lax.fori_loop(0, length // span, one, 0)

            inputs = pieces[0]
            if count > 1:
                inputs = x_s
                for i, piece in enumerate(pieces):
                    begin = pl.multiple_of(info[2 + i] * piece.shape[0], piece.shape[0])
                    x_s[pl.ds(begin, piece.shape[0]), :] = piece[...]

            zero = jnp.zeros((pad, width), F32)
            glu_s[0:pad, :] = zero
            glu_s[pad + length : pad + length + pad, :] = zero

            def ffn_norm(at):
                norm_s[at, :] = normalize(inputs[at, :].astype(F32), small[0:1, :]).astype(BF16)

            rows_loop(ffn_norm)
            for j in range(0, hidden, cols):
                part = dot(norm_s[...], up[0, :, j : j + cols])
                inner_s[:, j : j + cols] = (part * sigmoid(part)).astype(BF16)
            for j in range(0, width, cols):
                part = dot(inner_s[...], down[0, :, j : j + cols])
                start_s[:, j : j + cols] = inputs[:, j : j + cols].astype(F32) + 0.5 * part

            def attn_norm(at):
                norm_s[at, :] = normalize(start_s[at, :], small[1:2, :]).astype(BF16)

            rows_loop(attn_norm)
            for weight, target in ((query, q_s), (key, k_s), (value, v_s)):
                for j in range(0, width, cols):
                    target[:, j : j + cols] = dot(norm_s[...], weight[0, :, j : j + cols]).astype(BF16)

            frames = info[1]
            seen = lax.broadcasted_iota(jnp.int32, (1, length), 1) < frames
            lane = lax.broadcasted_iota(jnp.int32, (1, LANES), 1)
            group = LANES // head
            scale = 1.0 / math.sqrt(head)

            def one_group(g, carry):
                at = pl.ds(pl.multiple_of(g * LANES, LANES), LANES)
                queries, keys, values = q_s[:, at], k_s[:, at], v_s[:, at]
                mixed = jnp.zeros((length, 2 * LANES), F32)
                for h in range(group):
                    mine = (lane >= h * head) & (lane < (h + 1) * head)
                    k_head = jnp.where(mine, keys, jnp.zeros_like(keys))
                    scores = lax.dot_general(
                        queries, k_head, (((1,), (1,)), ((), ())), preferred_element_type=F32
                    )
                    scores = jnp.where(seen, scores, -1e30)
                    peak = jnp.max(scores, axis=-1, keepdims=True)
                    weights = jnp.exp2((scores - peak) * (scale * math.log2(math.e))).astype(BF16)
                    v_head = jnp.where(mine, values, jnp.zeros_like(values))
                    ones = jnp.broadcast_to(jnp.where(mine, 1.0, 0.0).astype(BF16), (length, LANES))
                    mixed = mixed + dot(weights, jnp.concatenate([v_head, ones], axis=1))
                norm_s[:, at] = (
                    mixed[:, :LANES] * pl.reciprocal(mixed[:, LANES:], approx=False)
                ).astype(BF16)
                return carry

            groups = width // LANES
            lax.fori_loop(0, groups, one_group, 0, unroll=UNROLL if length <= 256 else 1)

            for j in range(0, width, cols):
                part = dot(norm_s[...], out[0, :, j : j + cols])
                start_s[:, j : j + cols] = start_s[:, j : j + cols] + part

            def conv_norm(at):
                norm_s[at, :] = normalize(start_s[at, :], small[2:3, :]).astype(BF16)

            rows_loop(conv_norm)
            keep = lax.broadcasted_iota(jnp.int32, (length, 1), 0) < frames
            rows = 64
            shift = pad - rim

            def conv(begin, at):
                wide = glu_s[pl.ds(begin, rows + 2 * pad), at]
                total = None
                for r in range(8):
                    taps = [o for o in range(shift, shift + kernel) if o % 8 == r]
                    extent = rows + 8 if r else rows
                    partial = None
                    for o in taps:
                        tap = small[pl.ds(6 + o - shift, 1), at]
                        term = wide[o - r : o - r + extent] * tap
                        partial = term if partial is None else partial + term
                    if r:
                        partial = pltpu.roll(partial, extent - r, 0)[:rows]
                    total = partial if total is None else total + partial
                depth_s[pl.ds(begin, rows), at] = total

            block_cols = cols // 2
            for j in range(0, width, block_cols):
                part = dot(norm_s[...], expand[0, :, j : j + block_cols])
                gate = dot(norm_s[...], expand[0, :, width + j : width + j + block_cols])
                glu = jnp.where(keep, part * sigmoid(gate), 0.0)
                glu_s[pad : pad + length, j : j + block_cols] = glu.astype(BF16).astype(F32)
                for c in range(j, j + block_cols, LANES):
                    for i in range(0, length, rows):
                        conv(i, pl.ds(c, LANES))

            def swish(at):
                shifted = normalize(depth_s[at, :], small[3:4, :]) + small[4:5, :]
                norm_s[at, :] = (shifted * sigmoid(shifted)).astype(BF16)

            rows_loop(swish)
            for j in range(0, width, cols):
                part = dot(norm_s[...], shrink[0, :, j : j + cols])
                start_s[:, j : j + cols] = start_s[:, j : j + cols] + part

            def closing(at):
                result[at, :] = normalize(start_s[at, :], small[5:6, :]).astype(BF16)

            rows_loop(closing)

    return run


UNROLL = 8


def block(info, pieces, small, weights, kept, heads, kernel):
    length, width = kept.shape
    count = len(pieces)
    hidden = weights[0].shape[2]
    cols = 512
    pad = 8 * ((kernel // 2 + 8) // 8)
    vmem = [
        ((length, width), BF16),
        ((length, hidden), BF16),
        ((length, width), F32),
        ((length, width), BF16),
        ((length, width), BF16),
        ((length, width), BF16),
        ((length + 2 * pad, width), F32),
        ((length, width), F32),
        ((length, width), BF16),
    ]
    local = pl.BlockSpec(memory_space=pltpu.VMEM)
    return pl.pallas_call(
        block_kernel(heads, kernel, cols, count),
        out_shape=jax.ShapeDtypeStruct((length, width), BF16),
        in_specs=[pl.BlockSpec(memory_space=pltpu.SMEM)] + [local] * (count + 2 + len(weights)),
        out_specs=local,
        scratch_shapes=[pltpu.VMEM(shape, kind) for shape, kind in vmem],
        input_output_aliases={count + 2 + len(weights): 0},
        compiler_params=pltpu.CompilerParams(vmem_limit_bytes=LIMIT),
        name="block",
    )(info, *pieces, small, *weights, kept)


LIMIT = 30 * 1024 * 1024


def prefetch(info, weights):
    count = len(weights)

    def run(info, *refs):
        sources, targets, sems = refs[:count], refs[count:-1], refs[-1]

        @pl.when(info[0] == 1)
        def active():
            copies = [
                pltpu.make_async_copy(a, b, sems.at[i])
                for i, (a, b) in enumerate(zip(sources, targets))
            ]
            for copy in copies:
                copy.start()
            for copy in copies:
                copy.wait()

    return pl.pallas_call(
        run,
        out_shape=[pltpu.VMEM(w.shape, w.dtype) for w in weights],
        in_specs=[pl.BlockSpec(memory_space=pltpu.SMEM)] + [pl.BlockSpec(memory_space=pl.ANY)] * count,
        out_specs=[pl.BlockSpec(memory_space=pltpu.VMEM)] * len(weights),
        scratch_shapes=[pltpu.SemaphoreType.DMA((len(weights),))],
        compiler_params=pltpu.CompilerParams(vmem_limit_bytes=1024 * 1024),
        name="prefetch",
    )(info, *weights)


def body(
    frames,
    lengths,
    ffn_gain,
    ffn_up,
    ffn_down,
    attn_gain,
    query_weight,
    key_weight,
    value_weight,
    out_weight,
    conv_gain,
    expand_weight,
    depth_weight,
    depth_gain,
    norm_shift,
    shrink_weight,
    final_gain,
):
    sections = lax.axis_size("section")
    section_index = lax.axis_index("section")
    group_index = lax.axis_index("tm")
    micro, rows, width = frames.shape
    peers = lax.axis_size("tm")
    share = peers // micro
    assert share * micro == peers
    utterance = group_index // share
    kernel = depth_weight.shape[1]
    weights = (
        ffn_up,
        ffn_down,
        query_weight,
        key_weight,
        value_weight,
        out_weight,
        expand_weight,
        shrink_weight,
    )
    small = jnp.concatenate(
        [ffn_gain, attn_gain, conv_gain, depth_gain, norm_shift, final_gain, depth_weight[0]]
    )
    small = jnp.pad(small, ((0, -small.shape[0] % 8), (0, 0)))
    length = jnp.sum(jnp.where(jnp.arange(micro, dtype=jnp.int32) == utterance, lengths, 0))
    pairs = [(i, i + 1) for i in range(sections - 1)]
    axes = ("section", "tm")

    def apply(step, pieces, places, kept):
        mine = (step == section_index).astype(jnp.int32)
        info = jnp.stack([mine, length, *places])
        return block(info, pieces, small, prefetch(info, weights), kept, HEADS, kernel)

    pieces = [lax.dynamic_index_in_dim(frames, utterance, 0, keepdims=False)]
    places = [group_index]
    for r in range(1, peers):
        target = (group_index + r) % peers
        part = lax.dynamic_index_in_dim(frames, target // share, 0, keepdims=False)
        pieces.append(lax.ppermute(part, axes, [(j, (j + r) % peers) for j in range(peers)]))
        places.append((group_index - r) % peers)
    kept = apply(0, pieces, places, jnp.zeros((rows * peers, width), frames.dtype))

    def tick(step, kept):
        return apply(step, [lax.ppermute(kept, "section", pairs)], [], kept)

    kept = lax.fori_loop(1, sections, tick, kept)

    def rows_of(index):
        return lax.dynamic_slice_in_dim(kept, index * rows, rows, 0)

    result = jnp.zeros((micro, rows, width), kept.dtype)
    result = lax.dynamic_update_index_in_dim(result, rows_of(group_index), utterance, 0)
    for q in range(1, micro):
        r = q * share
        part = lax.ppermute(
            rows_of((group_index + r) % peers), "tm", [(j, (j + r) % peers) for j in range(peers)]
        )
        source = (group_index - r) % peers // share
        result = lax.dynamic_update_index_in_dim(result, part, source, 0)
    return result[None]


def solution(mesh):
    return jax.shard_map(
        body,
        mesh=mesh,
        in_specs=(
            P(None, "tm", None),
            P(),
            P("section", None),
            P("section", None, None),
            P("section", None, None),
            P("section", None),
            P("section", None, None),
            P("section", None, None),
            P("section", None, None),
            P("section", None, None),
            P("section", None),
            P("section", None, None),
            P("section", None, None),
            P("section", None),
            P("section", None),
            P("section", None, None),
            P("section", None),
        ),
        out_specs=P("section", None, "tm", None),
        check_vma=False,
    )
```

```python
import math

import jax
import jax.numpy as jnp
from jax import lax
from jax.experimental import pallas as pl
from jax.experimental.pallas import tpu as pltpu
from jax.sharding import PartitionSpec as P

HEADS = 16
EPS = 1e-05
LANES = 128
F32 = jnp.float32
BF16 = jnp.bfloat16


def sigmoid(value):
    return 0.5 * jnp.tanh(0.5 * value) + 0.5


def normalize(value, gain):
    mean = jnp.mean(value, axis=-1, keepdims=True)
    centred = value - mean
    spread = jnp.mean(centred * centred, axis=-1, keepdims=True)
    return centred * lax.rsqrt(spread + EPS) * gain


def dot(left, right):
    return jnp.dot(left, right, preferred_element_type=F32)


UP, DOWN, QUERY, KEY, VALUE, OUT, EXPAND, SHRINK = range(8)
COLS = 512


def pieces_of(index, shape):
    if index in (UP, DOWN):
        return [(0, slice(None), pl.ds(j, COLS)) for j in range(0, shape[2], COLS)]
    return [(0,)]


def block_kernel(heads, count, held, utterance_of, first, places):
    def run(*refs):
        refs = list(refs)

        def take(n):
            taken = refs[:n]
            del refs[:n]
            return taken

        (step, lengths) = take(2)
        pieces = take(count)
        params = take(held)
        take(1)
        (result,) = take(1)
        (norm_s, inner_s, start_s, q_s, k_s, v_s, glu_s, depth_s) = take(8)
        cols = COLS
        length, width = result.shape
        hidden = inner_s.shape[1]
        head = width // heads
        pad = (glu_s.shape[1] - length) // 2
        utterance = utterance_of()
        mine = lax.axis_index("section") == (0 if first else step[0])

        @pl.when(mine)
        def active():
            step_rows = 32
            span = min(length, 256)

            def rows_loop(fn):
                def one(i, carry):
                    for j in range(0, span, step_rows):
                        begin = j if span == length else pl.multiple_of(i * span + j, step_rows)
                        fn(pl.ds(begin, step_rows))
                    return carry

                if span == length:
                    one(0, 0)
                else:
                    lax.fori_loop(0, length // span, one, 0)

            inputs = pieces[0]
            local = params
            copies = {}
            if first:
                (inputs,) = take(1)
                local = take(held)
                (sems,) = take(1)
                order = list(range(8, held)) + list(range(8))
                for index in order:
                    shape = params[index].shape
                    parts = pieces_of(index, shape) if index < 8 else [(0,)]
                    for part in parts:
                        copy = pltpu.make_async_copy(
                            params[index].at[part],
                            local[index].at[part],
                            sems.at[sum(map(len, copies.values()))],
                        )
                        copy.start()
                        copies.setdefault(index, []).append(copy)
                for i, piece in enumerate(pieces):
                    begin = pl.multiple_of(places(i) * piece.shape[0], piece.shape[0])
                    inputs[pl.ds(begin, piece.shape[0]), :] = piece[...]
                for index in range(8, held):
                    copies[index][0].wait()

            def wait(index, column=0):
                if first and column // COLS < len(copies[index]):
                    copies[index][column // COLS].wait()

            weights = local[:8]
            (up, down, query, key, value, out, expand, shrink) = weights
            gains = local[8:14]
            taps = local[14]
            kernel = taps.shape[1]
            rim = kernel // 2

            zero = jnp.zeros((width // LANES, pad, LANES), F32)
            glu_s[:, 0:pad, :] = zero
            glu_s[:, pad + length : pad + length + pad, :] = zero

            def ffn_norm(at):
                norm_s[at, :] = normalize(inputs[at, :].astype(F32), gains[0][...]).astype(BF16)

            rows_loop(ffn_norm)
            for j in range(0, hidden, cols):
                wait(UP, j)
                part = dot(norm_s[...], up[0, :, j : j + cols])
                inner_s[:, j : j + cols] = (part * sigmoid(part)).astype(BF16)
            for j in range(0, width, cols):
                wait(DOWN, j)
                part = dot(inner_s[...], down[0, :, j : j + cols])
                start_s[:, j : j + cols] = inputs[:, j : j + cols].astype(F32) + 0.5 * part

            def attn_norm(at):
                norm_s[at, :] = normalize(start_s[at, :], gains[1][...]).astype(BF16)

            rows_loop(attn_norm)
            for which, target in ((QUERY, q_s), (KEY, k_s), (VALUE, v_s)):
                weight = weights[which]
                wait(which)
                for j in range(0, width, cols):
                    target[:, j : j + cols] = dot(norm_s[...], weight[0, :, j : j + cols]).astype(BF16)

            frames = lengths[utterance]
            seen = lax.broadcasted_iota(jnp.int32, (1, length), 1) < frames
            lane = lax.broadcasted_iota(jnp.int32, (1, LANES), 1)
            group = LANES // head
            scale = 1.0 / math.sqrt(head)

            def one_group(g, carry):
                at = pl.ds(pl.multiple_of(g * LANES, LANES), LANES)
                queries, keys, values = q_s[:, at], k_s[:, at], v_s[:, at]
                mixed = jnp.zeros((length, 2 * LANES), F32)
                for h in range(group):
                    mine = (lane >= h * head) & (lane < (h + 1) * head)
                    k_head = jnp.where(mine, keys, jnp.zeros_like(keys))
                    scores = lax.dot_general(
                        queries, k_head, (((1,), (1,)), ((), ())), preferred_element_type=F32
                    )
                    scores = jnp.where(seen, scores, -1e30)
                    peak = jnp.max(scores, axis=-1, keepdims=True)
                    weights = jnp.exp2((scores - peak) * (scale * math.log2(math.e))).astype(BF16)
                    v_head = jnp.where(mine, values, jnp.zeros_like(values))
                    ones = jnp.broadcast_to(jnp.where(mine, 1.0, 0.0).astype(BF16), (length, LANES))
                    mixed = mixed + dot(weights, jnp.concatenate([v_head, ones], axis=1))
                norm_s[:, at] = (
                    mixed[:, :LANES] * pl.reciprocal(mixed[:, LANES:], approx=False)
                ).astype(BF16)
                return carry

            groups = width // LANES
            lax.fori_loop(0, groups, one_group, 0, unroll=UNROLL if length <= 256 else 1)

            wait(OUT)
            for j in range(0, width, cols):
                part = dot(norm_s[...], out[0, :, j : j + cols])
                start_s[:, j : j + cols] = start_s[:, j : j + cols] + part

            def conv_norm(at):
                norm_s[at, :] = normalize(start_s[at, :], gains[2][...]).astype(BF16)

            rows_loop(conv_norm)
            keep = lax.broadcasted_iota(jnp.int32, (length, 1), 0) < frames
            rows = 256
            shift = pad - rim

            def conv(begin, slab):
                at = pl.ds(pl.multiple_of(slab * LANES, LANES), LANES)
                total = None
                for r in range(8):
                    offsets = range(r, kernel, 8)
                    wide = glu_s[slab, pl.ds(begin + shift + r, rows + 8 * (len(offsets) - 1)), :]
                    for i, o in enumerate(offsets):
                        term = wide[8 * i : 8 * i + rows] * taps[0, pl.ds(o, 1), at]
                        total = term if total is None else total + term
                depth_s[pl.ds(begin, rows), at] = total

            block_cols = cols // 2
            wait(EXPAND)
            for j in range(0, width, block_cols):
                part = dot(norm_s[...], expand[0, :, j : j + block_cols])
                gate = dot(norm_s[...], expand[0, :, width + j : width + j + block_cols])
                glu = jnp.where(keep, part * sigmoid(gate), 0.0)
                glu = glu.astype(BF16).astype(F32)
                for c in range(0, block_cols, LANES):
                    slab = (j + c) // LANES
                    glu_s[slab, pad : pad + length, :] = glu[:, c : c + LANES]

            chunks = length // rows

            def conv_step(i, carry):
                conv(pl.multiple_of(i % chunks * rows, rows), i // chunks)
                return carry

            lax.fori_loop(0, chunks * (width // LANES), conv_step, 0)

            def swish(at):
                shifted = normalize(depth_s[at, :], gains[3][...]) + gains[4][...]
                norm_s[at, :] = (shifted * sigmoid(shifted)).astype(BF16)

            rows_loop(swish)
            wait(SHRINK)
            for j in range(0, width, cols):
                part = dot(norm_s[...], shrink[0, :, j : j + cols])
                start_s[:, j : j + cols] = start_s[:, j : j + cols] + part

            def closing(at):
                result[at, :] = normalize(start_s[at, :], gains[5][...]).astype(BF16)

            rows_loop(closing)

    return run


UNROLL = 8


def block(step, lengths, places, pieces, params, kept, heads, utterance_of):
    length, width = kept.shape
    hidden = params[UP].shape[2]
    kernel = params[14].shape[1]
    count, held, first = len(pieces), len(params), step is None
    pad = 8 * ((kernel // 2 + 8) // 8)
    vmem = [
        ((length, width), BF16),
        ((length, hidden), BF16),
        ((length, width), F32),
        ((length, width), BF16),
        ((length, width), BF16),
        ((length, width), BF16),
        ((width // LANES, length + 2 * pad, LANES), F32),
        ((length, width), F32),
    ]
    scalars = [jnp.zeros((1,), jnp.int32) if first else step, lengths]
    sems = []
    if first:
        vmem += [((length, width), BF16)] + [(p.shape, p.dtype) for p in params]
        total = held - 8 + sum(len(pieces_of(i, params[i].shape)) for i in range(8))
        sems = [pltpu.SemaphoreType.DMA((total,))]
    local = pl.BlockSpec(memory_space=pltpu.VMEM)
    return pl.pallas_call(
        block_kernel(heads, count, held, utterance_of, first, places),
        out_shape=jax.ShapeDtypeStruct((length, width), BF16),
        in_specs=[pl.BlockSpec(memory_space=pltpu.SMEM)] * len(scalars)
        + [local] * count
        + [pl.BlockSpec(memory_space=pl.ANY) if first else local] * held
        + [local],
        out_specs=local,
        scratch_shapes=[pltpu.VMEM(shape, kind) for shape, kind in vmem] + sems,
        input_output_aliases={len(scalars) + count + held: 0},
        compiler_params=pltpu.CompilerParams(
            vmem_limit_bytes=(40 if first else 30) * 1024 * 1024
        ),
        name="block",
    )(*scalars, *pieces, *params, kept)


def prefetch(step, params):
    count = len(params)

    def run(step, *refs):
        sources, targets, sems = refs[:count], refs[count:-1], refs[-1]

        @pl.when(lax.axis_index("section") == step[0])
        def active():
            copies = [
                pltpu.make_async_copy(a, b, sems.at[i])
                for i, (a, b) in enumerate(zip(sources, targets))
            ]
            for copy in copies:
                copy.start()
            for copy in copies:
                copy.wait()

    return pl.pallas_call(
        run,
        out_shape=[pltpu.VMEM(p.shape, p.dtype) for p in params],
        in_specs=[pl.BlockSpec(memory_space=pltpu.SMEM)] + [pl.BlockSpec(memory_space=pl.ANY)] * count,
        out_specs=[pl.BlockSpec(memory_space=pltpu.VMEM)] * count,
        scratch_shapes=[pltpu.SemaphoreType.DMA((count,))],
        compiler_params=pltpu.CompilerParams(vmem_limit_bytes=1024 * 1024),
        name="prefetch",
    )(step, *params)


def body(
    frames,
    lengths,
    ffn_gain,
    ffn_up,
    ffn_down,
    attn_gain,
    query_weight,
    key_weight,
    value_weight,
    out_weight,
    conv_gain,
    expand_weight,
    depth_weight,
    depth_gain,
    norm_shift,
    shrink_weight,
    final_gain,
):
    sections = lax.axis_size("section")
    group_index = lax.axis_index("tm")
    micro, rows, width = frames.shape
    peers = lax.axis_size("tm")
    share = peers // micro
    assert share * micro == peers
    utterance = group_index // share
    params = (
        ffn_up,
        ffn_down,
        query_weight,
        key_weight,
        value_weight,
        out_weight,
        expand_weight,
        shrink_weight,
        ffn_gain,
        attn_gain,
        conv_gain,
        depth_gain,
        norm_shift,
        final_gain,
        depth_weight,
    )
    pairs = [(i, i + 1) for i in range(sections - 1)]
    axes = ("section", "tm")

    def utterance_of():
        return lax.axis_index("tm") // share

    def source_of(r):
        return lax.rem(lax.axis_index("tm") + (peers - r), peers)

    pieces = [lax.dynamic_index_in_dim(frames, utterance, 0, keepdims=False)]
    for r in range(1, peers):
        target = (group_index + r) % peers
        part = lax.dynamic_index_in_dim(frames, target // share, 0, keepdims=False)
        pieces.append(lax.ppermute(part, axes, [(j, (j + r) % peers) for j in range(peers)]))
    kept = jnp.zeros((rows * peers, width), frames.dtype)
    kept = block(None, lengths, source_of, pieces, params, kept, HEADS, utterance_of)

    def tick(step, kept):
        step = jnp.reshape(step, (1,))
        pieces = [lax.ppermute(kept, "section", pairs)]
        held = prefetch(step, params)
        return block(step, lengths, None, pieces, held, kept, HEADS, utterance_of)

    kept = lax.fori_loop(1, sections, tick, kept)

    def rows_of(index):
        return lax.dynamic_slice_in_dim(kept, index * rows, rows, 0)

    result = jnp.zeros((micro, rows, width), kept.dtype)
    result = lax.dynamic_update_index_in_dim(result, rows_of(group_index), utterance, 0)
    for q in range(1, micro):
        r = q * share
        part = lax.ppermute(
            rows_of((group_index + r) % peers), "tm", [(j, (j + r) % peers) for j in range(peers)]
        )
        source = (group_index - r) % peers // share
        result = lax.dynamic_update_index_in_dim(result, part, source, 0)
    return result[None]


def solution(mesh):
    return jax.shard_map(
        body,
        mesh=mesh,
        in_specs=(
            P(None, "tm", None),
            P(),
            P("section", None),
            P("section", None, None),
            P("section", None, None),
            P("section", None),
            P("section", None, None),
            P("section", None, None),
            P("section", None, None),
            P("section", None, None),
            P("section", None),
            P("section", None, None),
            P("section", None, None),
            P("section", None),
            P("section", None),
            P("section", None, None),
            P("section", None),
        ),
        out_specs=P("section", None, "tm", None),
        check_vma=False,
    )
```

```python
import math

import jax
import jax.numpy as jnp
from jax import lax
from jax.experimental import pallas as pl
from jax.experimental.pallas import tpu as pltpu
from jax.sharding import PartitionSpec as P

HEADS = 16
EPS = 1e-05
LANES = 128
F32 = jnp.float32
BF16 = jnp.bfloat16


def sigmoid(value):
    return 0.5 * jnp.tanh(0.5 * value) + 0.5


def normalize(value, gain):
    mean = jnp.mean(value, axis=-1, keepdims=True)
    centred = value - mean
    spread = jnp.mean(centred * centred, axis=-1, keepdims=True)
    return centred * lax.rsqrt(spread + EPS) * gain


def dot(left, right):
    return jnp.dot(left, right, preferred_element_type=F32)


UP, DOWN, QUERY, KEY, VALUE, OUT, EXPAND, SHRINK = range(8)
COLS = 512


def pieces_of(index, shape):
    if index in (UP, DOWN):
        return [(0, slice(None), pl.ds(j, COLS)) for j in range(0, shape[2], COLS)]
    return [(0,)]


def block_kernel(heads, count, held, utterance_of, first, places):
    def run(*refs):
        refs = list(refs)

        def take(n):
            taken = refs[:n]
            del refs[:n]
            return taken

        (step, lengths) = take(2)
        pieces = take(count)
        params = take(held)
        take(1)
        (result,) = take(1)
        (norm_s, inner_s, start_s, q_s, k_s, v_s, glu_s, depth_s) = take(8)
        cols = COLS
        length, width = result.shape
        hidden = inner_s.shape[1]
        head = width // heads
        pad = (glu_s.shape[1] - length) // 2
        utterance = utterance_of()
        mine = lax.axis_index("section") == (0 if first else step[0])

        @pl.when(mine)
        def active():
            step_rows = 32
            span = min(length, 256)

            def rows_loop(fn):
                def one(i, carry):
                    for j in range(0, span, step_rows):
                        begin = j if span == length else pl.multiple_of(i * span + j, step_rows)
                        fn(pl.ds(begin, step_rows))
                    return carry

                if span == length:
                    one(0, 0)
                else:
                    lax.fori_loop(0, length // span, one, 0)

            inputs = pieces[0]
            local = params
            copies = {}
            if first:
                (assembled,) = take(1)
                inputs = assembled if count > 1 else inputs
                local = take(held)
                (sems,) = take(1)
                order = list(range(8, held)) + list(range(8))
                for index in order:
                    shape = params[index].shape
                    parts = pieces_of(index, shape) if index < 8 else [(0,)]
                    for part in parts:
                        copy = pltpu.make_async_copy(
                            params[index].at[part],
                            local[index].at[part],
                            sems.at[sum(map(len, copies.values()))],
                        )
                        copy.start()
                        copies.setdefault(index, []).append(copy)
                for i, piece in enumerate(pieces if count > 1 else []):
                    begin = pl.multiple_of(places(i) * piece.shape[0], piece.shape[0])
                    assembled[pl.ds(begin, piece.shape[0]), :] = piece[...]
                for index in range(8, held):
                    copies[index][0].wait()

            def wait(index, column=0):
                if first and column // COLS < len(copies[index]):
                    copies[index][column // COLS].wait()

            weights = local[:8]
            (up, down, query, key, value, out, expand, shrink) = weights
            gains = local[8:14]
            taps = local[14]
            kernel = taps.shape[1]
            rim = kernel // 2

            zero = jnp.zeros((width // LANES, pad, LANES), F32)
            glu_s[:, 0:pad, :] = zero
            glu_s[:, pad + length : pad + length + pad, :] = zero

            def ffn_norm(at):
                norm_s[at, :] = normalize(inputs[at, :].astype(F32), gains[0][...]).astype(BF16)

            rows_loop(ffn_norm)
            for j in range(0, hidden, cols):
                wait(UP, j)
                part = dot(norm_s[...], up[0, :, j : j + cols])
                inner_s[:, j : j + cols] = (part * sigmoid(part)).astype(BF16)
            for j in range(0, width, cols):
                wait(DOWN, j)
                part = dot(inner_s[...], down[0, :, j : j + cols])
                start_s[:, j : j + cols] = inputs[:, j : j + cols].astype(F32) + 0.5 * part

            def attn_norm(at):
                norm_s[at, :] = normalize(start_s[at, :], gains[1][...]).astype(BF16)

            rows_loop(attn_norm)
            for which, target in ((QUERY, q_s), (KEY, k_s), (VALUE, v_s)):
                weight = weights[which]
                wait(which)
                for j in range(0, width, cols):
                    part = dot(norm_s[...], weight[0, :, j : j + cols])
                    if which == QUERY:
                        part = part * (math.log2(math.e) / math.sqrt(head))
                    target[:, j : j + cols] = part.astype(BF16)

            frames = lengths[utterance]
            seen = lax.broadcasted_iota(jnp.int32, (1, length), 1) < frames
            lane = lax.broadcasted_iota(jnp.int32, (1, LANES), 1)
            group = LANES // head

            def one_group(g, carry):
                at = pl.ds(pl.multiple_of(g * LANES, LANES), LANES)
                queries, keys, values = q_s[:, at], k_s[:, at], v_s[:, at]
                mixed = jnp.zeros((length, 2 * LANES), F32)
                for h in range(group):
                    mine = (lane >= h * head) & (lane < (h + 1) * head)
                    k_head = jnp.where(mine, keys, jnp.zeros_like(keys))
                    scores = lax.dot_general(
                        queries, k_head, (((1,), (1,)), ((), ())), preferred_element_type=F32
                    )
                    scores = jnp.where(seen, scores, -1e30)
                    peak = jnp.max(scores, axis=-1, keepdims=True)
                    weights = jnp.exp2(scores - peak).astype(BF16)
                    v_head = jnp.where(mine, values, jnp.zeros_like(values))
                    ones = jnp.broadcast_to(jnp.where(mine, 1.0, 0.0).astype(BF16), (length, LANES))
                    mixed = mixed + dot(weights, jnp.concatenate([v_head, ones], axis=1))
                norm_s[:, at] = (
                    mixed[:, :LANES] * pl.reciprocal(mixed[:, LANES:], approx=False)
                ).astype(BF16)
                return carry

            groups = width // LANES
            lax.fori_loop(0, groups, one_group, 0, unroll=UNROLL if length <= 256 else 1)

            wait(OUT)
            for j in range(0, width, cols):
                part = dot(norm_s[...], out[0, :, j : j + cols])
                start_s[:, j : j + cols] = start_s[:, j : j + cols] + part

            def conv_norm(at):
                norm_s[at, :] = normalize(start_s[at, :], gains[2][...]).astype(BF16)

            rows_loop(conv_norm)
            keep = lax.broadcasted_iota(jnp.int32, (length, 1), 0) < frames
            rows = 256
            shift = pad - rim

            def conv(begin, slab):
                at = pl.ds(pl.multiple_of(slab * LANES, LANES), LANES)
                total = None
                for r in range(8):
                    offsets = range(r, kernel, 8)
                    wide = glu_s[slab, pl.ds(begin + shift + r, rows + 8 * (len(offsets) - 1)), :]
                    for i, o in enumerate(offsets):
                        term = wide[8 * i : 8 * i + rows] * taps[0, pl.ds(o, 1), at]
                        total = term if total is None else total + term
                depth_s[pl.ds(begin, rows), at] = total

            block_cols = cols // 2
            wait(EXPAND)
            for j in range(0, width, block_cols):
                part = dot(norm_s[...], expand[0, :, j : j + block_cols])
                gate = dot(norm_s[...], expand[0, :, width + j : width + j + block_cols])
                glu = jnp.where(keep, part * sigmoid(gate), 0.0)
                glu = glu.astype(BF16).astype(F32)
                for c in range(0, block_cols, LANES):
                    slab = (j + c) // LANES
                    glu_s[slab, pad : pad + length, :] = glu[:, c : c + LANES]

            chunks = length // rows

            def conv_step(i, carry):
                conv(pl.multiple_of(i % chunks * rows, rows), i // chunks)
                return carry

            lax.fori_loop(0, chunks * (width // LANES), conv_step, 0)

            def swish(at):
                shifted = normalize(depth_s[at, :], gains[3][...]) + gains[4][...]
                norm_s[at, :] = (shifted * sigmoid(shifted)).astype(BF16)

            rows_loop(swish)
            wait(SHRINK)
            for j in range(0, width, cols):
                part = dot(norm_s[...], shrink[0, :, j : j + cols])
                start_s[:, j : j + cols] = start_s[:, j : j + cols] + part

            def closing(at):
                result[at, :] = normalize(start_s[at, :], gains[5][...]).astype(BF16)

            rows_loop(closing)

    return run


UNROLL = 8


def block(step, lengths, places, pieces, params, kept, heads, utterance_of):
    length, width = kept.shape
    hidden = params[UP].shape[2]
    kernel = params[14].shape[1]
    count, held, first = len(pieces), len(params), step is None
    pad = 8 * ((kernel // 2 + 8) // 8)
    vmem = [
        ((length, width), BF16),
        ((length, hidden), BF16),
        ((length, width), F32),
        ((length, width), BF16),
        ((length, width), BF16),
        ((length, width), BF16),
        ((width // LANES, length + 2 * pad, LANES), F32),
        ((length, width), F32),
    ]
    scalars = [jnp.zeros((1,), jnp.int32) if first else step, lengths]
    sems = []
    if first:
        vmem += [((length, width), BF16)] + [(p.shape, p.dtype) for p in params]
        total = held - 8 + sum(len(pieces_of(i, params[i].shape)) for i in range(8))
        sems = [pltpu.SemaphoreType.DMA((total,))]
    local = pl.BlockSpec(memory_space=pltpu.VMEM)
    return pl.pallas_call(
        block_kernel(heads, count, held, utterance_of, first, places),
        out_shape=jax.ShapeDtypeStruct((length, width), BF16),
        in_specs=[pl.BlockSpec(memory_space=pltpu.SMEM)] * len(scalars)
        + [local] * count
        + [pl.BlockSpec(memory_space=pl.ANY) if first else local] * held
        + [local],
        out_specs=local,
        scratch_shapes=[pltpu.VMEM(shape, kind) for shape, kind in vmem] + sems,
        input_output_aliases={len(scalars) + count + held: 0},
        compiler_params=pltpu.CompilerParams(
            vmem_limit_bytes=(40 if first else 30) * 1024 * 1024
        ),
        name="block",
    )(*scalars, *pieces, *params, kept)


def prefetch(step, params):
    count = len(params)

    def run(step, *refs):
        sources, targets, sems = refs[:count], refs[count:-1], refs[-1]

        @pl.when(lax.axis_index("section") == step[0])
        def active():
            copies = [
                pltpu.make_async_copy(a, b, sems.at[i])
                for i, (a, b) in enumerate(zip(sources, targets))
            ]
            for copy in copies:
                copy.start()
            for copy in copies:
                copy.wait()

    return pl.pallas_call(
        run,
        out_shape=[pltpu.VMEM(p.shape, p.dtype) for p in params],
        in_specs=[pl.BlockSpec(memory_space=pltpu.SMEM)] + [pl.BlockSpec(memory_space=pl.ANY)] * count,
        out_specs=[pl.BlockSpec(memory_space=pltpu.VMEM)] * count,
        scratch_shapes=[pltpu.SemaphoreType.DMA((count,))],
        compiler_params=pltpu.CompilerParams(vmem_limit_bytes=1024 * 1024),
        name="prefetch",
    )(step, *params)


def body(
    frames,
    lengths,
    ffn_gain,
    ffn_up,
    ffn_down,
    attn_gain,
    query_weight,
    key_weight,
    value_weight,
    out_weight,
    conv_gain,
    expand_weight,
    depth_weight,
    depth_gain,
    norm_shift,
    shrink_weight,
    final_gain,
):
    sections = lax.axis_size("section")
    group_index = lax.axis_index("tm")
    micro, rows, width = frames.shape
    peers = lax.axis_size("tm")
    share = peers // micro
    assert share * micro == peers
    utterance = group_index // share
    params = (
        ffn_up,
        ffn_down,
        query_weight,
        key_weight,
        value_weight,
        out_weight,
        expand_weight,
        shrink_weight,
        ffn_gain,
        attn_gain,
        conv_gain,
        depth_gain,
        norm_shift,
        final_gain,
        depth_weight,
    )
    pairs = [(i, i + 1) for i in range(sections - 1)]
    axes = ("section", "tm")

    def utterance_of():
        return lax.axis_index("tm") // share

    def source_of(r):
        return lax.rem(lax.axis_index("tm") + (peers - r), peers)

    if share == 1:
        own = lax.all_to_all(frames, "tm", 0, 0, tiled=True)
        pieces = [own.reshape(rows * peers, width)]
    else:
        pieces = [lax.dynamic_index_in_dim(frames, utterance, 0, keepdims=False)]
        for r in range(1, peers):
            target = (group_index + r) % peers
            part = lax.dynamic_index_in_dim(frames, target // share, 0, keepdims=False)
            pieces.append(lax.ppermute(part, axes, [(j, (j + r) % peers) for j in range(peers)]))
    kept = jnp.zeros((rows * peers, width), frames.dtype)
    kept = block(None, lengths, source_of, pieces, params, kept, HEADS, utterance_of)

    def tick(step, kept):
        step = jnp.reshape(step, (1,))
        pieces = [lax.ppermute(kept, "section", pairs)]
        held = prefetch(step, params)
        return block(step, lengths, None, pieces, held, kept, HEADS, utterance_of)

    kept = lax.fori_loop(1, sections, tick, kept)

    def rows_of(index):
        return lax.dynamic_slice_in_dim(kept, index * rows, rows, 0)

    result = jnp.zeros((micro, rows, width), kept.dtype)
    result = lax.dynamic_update_index_in_dim(result, rows_of(group_index), utterance, 0)
    for q in range(1, micro):
        r = q * share
        part = lax.ppermute(
            rows_of((group_index + r) % peers), "tm", [(j, (j + r) % peers) for j in range(peers)]
        )
        source = (group_index - r) % peers // share
        result = lax.dynamic_update_index_in_dim(result, part, source, 0)
    return result[None]


def solution(mesh):
    return jax.shard_map(
        body,
        mesh=mesh,
        in_specs=(
            P(None, "tm", None),
            P(),
            P("section", None),
            P("section", None, None),
            P("section", None, None),
            P("section", None),
            P("section", None, None),
            P("section", None, None),
            P("section", None, None),
            P("section", None, None),
            P("section", None),
            P("section", None, None),
            P("section", None, None),
            P("section", None),
            P("section", None),
            P("section", None, None),
            P("section", None),
        ),
        out_specs=P("section", None, "tm", None),
        check_vma=False,
    )
```

```python
import math

import jax
import jax.numpy as jnp
from jax import lax
from jax.experimental import pallas as pl
from jax.experimental.pallas import tpu as pltpu
from jax.sharding import PartitionSpec as P

HEADS = 16
EPS = 1e-05
LANES = 128
F32 = jnp.float32
BF16 = jnp.bfloat16


def sigmoid(value):
    return 0.5 * jnp.tanh(0.5 * value) + 0.5


def normalize(value, gain):
    mean = jnp.mean(value, axis=-1, keepdims=True)
    centred = value - mean
    spread = jnp.mean(centred * centred, axis=-1, keepdims=True)
    return centred * lax.rsqrt(spread + EPS) * gain


def dot(left, right):
    return jnp.dot(left, right, preferred_element_type=F32)


UP, DOWN, QUERY, KEY, VALUE, OUT, EXPAND, SHRINK = range(8)
COLS = 512
WINDOW = 5 * 1024 * 1024


def pieces_of(index, shape):
    if index in (UP, DOWN):
        return [(0, slice(None), pl.ds(j, COLS)) for j in range(0, shape[2], COLS)]
    return [(0,)]


def block_kernel(heads, count, held, utterance_of, first, places):
    def run(*refs):
        refs = list(refs)

        def take(n):
            taken = refs[:n]
            del refs[:n]
            return taken

        (step, lengths) = take(2)
        pieces = take(count)
        params = take(held)
        take(1)
        (result,) = take(1)
        (norm_s, inner_s, start_s, q_s, k_s, v_s, glu_s, depth_s) = take(8)
        cols = COLS
        length, width = result.shape
        hidden = inner_s.shape[1]
        head = width // heads
        pad = (glu_s.shape[1] - length) // 2
        utterance = utterance_of()
        mine = lax.axis_index("section") == (0 if first else step[0])

        @pl.when(mine)
        def active():
            step_rows = 32
            span = min(length, 256)

            def rows_loop(fn):
                def one(i, carry):
                    for j in range(0, span, step_rows):
                        begin = j if span == length else pl.multiple_of(i * span + j, step_rows)
                        fn(pl.ds(begin, step_rows))
                    return carry

                if span == length:
                    one(0, 0)
                else:
                    lax.fori_loop(0, length // span, one, 0)

            inputs = pieces[0]
            local = params
            copies = {}
            if first:
                (assembled,) = take(1)
                inputs = assembled if count > 1 else inputs
                local = take(held)
                (sems,) = take(1)
                items = [
                    (index, part)
                    for index in range(8)
                    for part in pieces_of(index, params[index].shape)
                ]
                early = [(index, (0,)) for index in range(8, held)]
                for number, (index, part) in enumerate(early + items):
                    copy = pltpu.make_async_copy(
                        params[index].at[part], local[index].at[part], sems.at[number]
                    )
                    copies.setdefault(index, []).append(copy)
                queue = [copy for index in range(8) for copy in copies[index]]
                sizes = [
                    2 * math.prod(params[index].shape) // len(copies[index])
                    for index in range(8)
                    for _ in copies[index]
                ]
                flight = {}

                def launch():
                    while queue and sum(flight.values()) < WINDOW:
                        copy = queue.pop(0)
                        copy.start()
                        flight[id(copy)] = sizes.pop(0)

                for index in range(8, held):
                    copies[index][0].start()
                launch()
                for i, piece in enumerate(pieces if count > 1 else []):
                    begin = pl.multiple_of(places(i) * piece.shape[0], piece.shape[0])
                    assembled[pl.ds(begin, piece.shape[0]), :] = piece[...]
                copies[8][0].wait()

            def wait(index, column=0):
                if first and column // COLS < len(copies[index]):
                    copy = copies[index][column // COLS]
                    copy.wait()
                    flight.pop(id(copy))
                    launch()

            weights = local[:8]
            (up, down, query, key, value, out, expand, shrink) = weights
            gains = local[8:14]
            taps = local[14]
            kernel = taps.shape[1]
            rim = kernel // 2

            zero = jnp.zeros((width // LANES, pad, LANES), F32)
            glu_s[:, 0:pad, :] = zero
            glu_s[:, pad + length : pad + length + pad, :] = zero

            def ffn_norm(at):
                norm_s[at, :] = normalize(inputs[at, :].astype(F32), gains[0][...]).astype(BF16)

            rows_loop(ffn_norm)
            for j in range(0, hidden, cols):
                wait(UP, j)
                part = dot(norm_s[...], up[0, :, j : j + cols])
                inner_s[:, j : j + cols] = (part * sigmoid(part)).astype(BF16)
            for j in range(0, width, cols):
                wait(DOWN, j)
                part = dot(inner_s[...], down[0, :, j : j + cols])
                start_s[:, j : j + cols] = inputs[:, j : j + cols].astype(F32) + 0.5 * part

            if first:
                for index in range(9, held):
                    copies[index][0].wait()

            def attn_norm(at):
                norm_s[at, :] = normalize(start_s[at, :], gains[1][...]).astype(BF16)

            rows_loop(attn_norm)
            for which, target in ((QUERY, q_s), (KEY, k_s), (VALUE, v_s)):
                weight = weights[which]
                wait(which)
                for j in range(0, width, cols):
                    part = dot(norm_s[...], weight[0, :, j : j + cols])
                    if which == QUERY:
                        part = part * (math.log2(math.e) / math.sqrt(head))
                    target[:, j : j + cols] = part.astype(BF16)

            frames = lengths[utterance]
            seen = lax.broadcasted_iota(jnp.int32, (1, length), 1) < frames
            lane = lax.broadcasted_iota(jnp.int32, (1, LANES), 1)
            group = LANES // head

            def one_group(g, carry):
                at = pl.ds(pl.multiple_of(g * LANES, LANES), LANES)
                queries, keys, values = q_s[:, at], k_s[:, at], v_s[:, at]
                mixed = jnp.zeros((length, 2 * LANES), F32)
                for h in range(group):
                    mine = (lane >= h * head) & (lane < (h + 1) * head)
                    k_head = jnp.where(mine, keys, jnp.zeros_like(keys))
                    scores = lax.dot_general(
                        queries, k_head, (((1,), (1,)), ((), ())), preferred_element_type=F32
                    )
                    scores = jnp.where(seen, scores, -1e30)
                    peak = jnp.max(scores, axis=-1, keepdims=True)
                    weights = jnp.exp2(scores - peak).astype(BF16)
                    v_head = jnp.where(mine, values, jnp.zeros_like(values))
                    ones = jnp.broadcast_to(jnp.where(mine, 1.0, 0.0).astype(BF16), (length, LANES))
                    mixed = mixed + dot(weights, jnp.concatenate([v_head, ones], axis=1))
                norm_s[:, at] = (
                    mixed[:, :LANES] * pl.reciprocal(mixed[:, LANES:], approx=False)
                ).astype(BF16)
                return carry

            groups = width // LANES
            lax.fori_loop(0, groups, one_group, 0, unroll=UNROLL if length <= 256 else 1)

            wait(OUT)
            for j in range(0, width, cols):
                part = dot(norm_s[...], out[0, :, j : j + cols])
                start_s[:, j : j + cols] = start_s[:, j : j + cols] + part

            def conv_norm(at):
                norm_s[at, :] = normalize(start_s[at, :], gains[2][...]).astype(BF16)

            rows_loop(conv_norm)
            keep = lax.broadcasted_iota(jnp.int32, (length, 1), 0) < frames
            rows = 256
            shift = pad - rim

            def conv(begin, slab):
                at = pl.ds(pl.multiple_of(slab * LANES, LANES), LANES)
                total = None
                for r in range(8):
                    offsets = range(r, kernel, 8)
                    wide = glu_s[slab, pl.ds(begin + shift + r, rows + 8 * (len(offsets) - 1)), :]
                    for i, o in enumerate(offsets):
                        term = wide[8 * i : 8 * i + rows] * taps[0, pl.ds(o, 1), at]
                        total = term if total is None else total + term
                depth_s[pl.ds(begin, rows), at] = total

            block_cols = cols // 2
            wait(EXPAND)
            for j in range(0, width, block_cols):
                part = dot(norm_s[...], expand[0, :, j : j + block_cols])
                gate = dot(norm_s[...], expand[0, :, width + j : width + j + block_cols])
                glu = jnp.where(keep, part * sigmoid(gate), 0.0)
                glu = glu.astype(BF16).astype(F32)
                for c in range(0, block_cols, LANES):
                    slab = (j + c) // LANES
                    glu_s[slab, pad : pad + length, :] = glu[:, c : c + LANES]

            chunks = length // rows

            def conv_step(i, carry):
                conv(pl.multiple_of(i % chunks * rows, rows), i // chunks)
                return carry

            lax.fori_loop(0, chunks * (width // LANES), conv_step, 0)

            def swish(at):
                shifted = normalize(depth_s[at, :], gains[3][...]) + gains[4][...]
                norm_s[at, :] = (shifted * sigmoid(shifted)).astype(BF16)

            rows_loop(swish)
            wait(SHRINK)
            for j in range(0, width, cols):
                part = dot(norm_s[...], shrink[0, :, j : j + cols])
                start_s[:, j : j + cols] = start_s[:, j : j + cols] + part

            def closing(at):
                result[at, :] = normalize(start_s[at, :], gains[5][...]).astype(BF16)

            rows_loop(closing)

    return run


UNROLL = 8


def block(step, lengths, places, pieces, params, kept, heads, utterance_of):
    length, width = kept.shape
    hidden = params[UP].shape[2]
    kernel = params[14].shape[1]
    count, held, first = len(pieces), len(params), step is None
    pad = 8 * ((kernel // 2 + 8) // 8)
    vmem = [
        ((length, width), BF16),
        ((length, hidden), BF16),
        ((length, width), F32),
        ((length, width), BF16),
        ((length, width), BF16),
        ((length, width), BF16),
        ((width // LANES, length + 2 * pad, LANES), F32),
        ((length, width), F32),
    ]
    scalars = [jnp.zeros((1,), jnp.int32) if first else step, lengths]
    sems = []
    if first:
        vmem += [((length, width), BF16)] + [(p.shape, p.dtype) for p in params]
        total = held - 8 + sum(len(pieces_of(i, params[i].shape)) for i in range(8))
        sems = [pltpu.SemaphoreType.DMA((total,))]
    local = pl.BlockSpec(memory_space=pltpu.VMEM)
    return pl.pallas_call(
        block_kernel(heads, count, held, utterance_of, first, places),
        out_shape=jax.ShapeDtypeStruct((length, width), BF16),
        in_specs=[pl.BlockSpec(memory_space=pltpu.SMEM)] * len(scalars)
        + [local] * count
        + [pl.BlockSpec(memory_space=pl.ANY) if first else local] * held
        + [local],
        out_specs=local,
        scratch_shapes=[pltpu.VMEM(shape, kind) for shape, kind in vmem] + sems,
        input_output_aliases={len(scalars) + count + held: 0},
        compiler_params=pltpu.CompilerParams(
            vmem_limit_bytes=(40 if first else 30) * 1024 * 1024
        ),
        name="block",
    )(*scalars, *pieces, *params, kept)


def prefetch(step, params):
    count = len(params)

    def run(step, *refs):
        sources, targets, sems = refs[:count], refs[count:-1], refs[-1]

        @pl.when(lax.axis_index("section") == step[0])
        def active():
            copies = [
                pltpu.make_async_copy(a, b, sems.at[i])
                for i, (a, b) in enumerate(zip(sources, targets))
            ]
            for copy in copies:
                copy.start()
            for copy in copies:
                copy.wait()

    return pl.pallas_call(
        run,
        out_shape=[pltpu.VMEM(p.shape, p.dtype) for p in params],
        in_specs=[pl.BlockSpec(memory_space=pltpu.SMEM)] + [pl.BlockSpec(memory_space=pl.ANY)] * count,
        out_specs=[pl.BlockSpec(memory_space=pltpu.VMEM)] * count,
        scratch_shapes=[pltpu.SemaphoreType.DMA((count,))],
        compiler_params=pltpu.CompilerParams(vmem_limit_bytes=1024 * 1024),
        name="prefetch",
    )(step, *params)


def body(
    frames,
    lengths,
    ffn_gain,
    ffn_up,
    ffn_down,
    attn_gain,
    query_weight,
    key_weight,
    value_weight,
    out_weight,
    conv_gain,
    expand_weight,
    depth_weight,
    depth_gain,
    norm_shift,
    shrink_weight,
    final_gain,
):
    sections = lax.axis_size("section")
    group_index = lax.axis_index("tm")
    micro, rows, width = frames.shape
    peers = lax.axis_size("tm")
    share = peers // micro
    assert share * micro == peers
    utterance = group_index // share
    params = (
        ffn_up,
        ffn_down,
        query_weight,
        key_weight,
        value_weight,
        out_weight,
        expand_weight,
        shrink_weight,
        ffn_gain,
        attn_gain,
        conv_gain,
        depth_gain,
        norm_shift,
        final_gain,
        depth_weight,
    )
    pairs = [(i, i + 1) for i in range(sections - 1)]
    axes = ("section", "tm")

    def utterance_of():
        return lax.axis_index("tm") // share

    def source_of(r):
        return lax.rem(lax.axis_index("tm") + (peers - r), peers)

    if share == 1:
        own = lax.all_to_all(frames, "tm", 0, 0, tiled=True)
        pieces = [own.reshape(rows * peers, width)]
    else:
        pieces = [lax.dynamic_index_in_dim(frames, utterance, 0, keepdims=False)]
        for r in range(1, peers):
            target = (group_index + r) % peers
            part = lax.dynamic_index_in_dim(frames, target // share, 0, keepdims=False)
            pieces.append(lax.ppermute(part, axes, [(j, (j + r) % peers) for j in range(peers)]))
    kept = jnp.zeros((rows * peers, width), frames.dtype)
    kept = block(None, lengths, source_of, pieces, params, kept, HEADS, utterance_of)

    def tick(step, kept):
        step = jnp.reshape(step, (1,))
        pieces = [lax.ppermute(kept, "section", pairs)]
        held = prefetch(step, params)
        return block(step, lengths, None, pieces, held, kept, HEADS, utterance_of)

    kept = lax.fori_loop(1, sections, tick, kept)

    def rows_of(index):
        return lax.dynamic_slice_in_dim(kept, index * rows, rows, 0)

    result = jnp.zeros((micro, rows, width), kept.dtype)
    result = lax.dynamic_update_index_in_dim(result, rows_of(group_index), utterance, 0)
    for q in range(1, micro):
        r = q * share
        part = lax.ppermute(
            rows_of((group_index + r) % peers), "tm", [(j, (j + r) % peers) for j in range(peers)]
        )
        source = (group_index - r) % peers // share
        result = lax.dynamic_update_index_in_dim(result, part, source, 0)
    return result[None]


def solution(mesh):
    return jax.shard_map(
        body,
        mesh=mesh,
        in_specs=(
            P(None, "tm", None),
            P(),
            P("section", None),
            P("section", None, None),
            P("section", None, None),
            P("section", None),
            P("section", None, None),
            P("section", None, None),
            P("section", None, None),
            P("section", None, None),
            P("section", None),
            P("section", None, None),
            P("section", None, None),
            P("section", None),
            P("section", None),
            P("section", None, None),
            P("section", None),
        ),
        out_specs=P("section", None, "tm", None),
        check_vma=False,
    )
```
